8 devices in a mesh: dp: 1 (over z), sub: 2 (over y), ep: 4 (over x, core).
Axes of the slice: x: 2, y: 2, z: 1, core: 2. Of those that a mesh axis runs over, the one named last changes fastest.
Arguments:
- input_a: bfloat16 [8, 512, 4096], P(('dp', 'ep', 'sub'))
- input_b: bfloat16 [8, 512, 4096], P(('dp', 'ep', 'sub'))
- route_idx: int32 [2, 4096, 8], P(None, ('dp', 'ep', 'sub'))
- route_gate: float32 [2, 4096, 8], P(None, ('dp', 'ep', 'sub'))
- attn_norm: float32 [4096], replicated
- w_query: bfloat16 [4096, 64, 128], replicated
- w_key: bfloat16 [4096, 64, 128], replicated
- w_value: bfloat16 [4096, 64, 128], replicated
- w_out: bfloat16 [64, 128, 4096], replicated
- moe_norm: float32 [4096], replicated
- w_gate: bfloat16 [16, 4096, 1536], P(('ep', 'sub'))
- w_up: bfloat16 [16, 4096, 1536], P(('ep', 'sub'))
- w_down: bfloat16 [16, 1536, 4096], P(('ep', 'sub'))
Outputs:
- output 1: bfloat16 [8, 512, 4096], P(('dp', 'ep', 'sub'))
- output 2: bfloat16 [8, 512, 4096], P(('dp', 'ep', 'sub'))
All inputs are finite; a program needn't handle non-finite values.
Results may differ from the reference program's by a relative error of at most 0.0126636.
Values are sent between devices in bfloat16 or wider.
A program may use at most 1.5 GiB of HBM per device.

```python
import functools
import jax
import jax.numpy as jnp
from jax import lax

MODEL_DIM = 4096
NUM_HEADS = 64
HEAD_DIM = 128
FF_DIM = 1536
TOP_K = 8
TOK_DEV = 512
SEQ_LEN = 512
EXP_LOCAL = 2
EP_SIZE = 4
SUB_SIZE = 2
NODE_LIM = 2

NUM_DEV = EP_SIZE * SUB_SIZE
NUM_EXP = EXP_LOCAL * NUM_DEV
NUM_TOK = NUM_DEV * TOK_DEV
NUM_SEQ = NUM_TOK // SEQ_LEN
CAP_SLOTS = 3 * TOP_K * TOK_DEV // (2 * NUM_EXP)
EXP_ROOM = NUM_DEV * CAP_SLOTS
NODE_EXP = SUB_SIZE * EXP_LOCAL
PER_VISIT = TOP_K // NODE_LIM
HOT_VISITS = 3 * NODE_LIM * TOK_DEV // (2 * EP_SIZE)
COLD_VISITS = NODE_LIM * TOK_DEV // (2 * EP_SIZE)
NORM_EPS = 1e-6


def draw_device_routes(rng_key):
    key_hot, key_tok, key_exp = jax.random.split(rng_key, 3)
    node_rank = jax.random.permutation(key_hot, jnp.arange(EP_SIZE))
    visits = jnp.where(node_rank < EP_SIZE // 2, HOT_VISITS, COLD_VISITS)
    run_ends = jnp.cumsum(visits)
    run_starts = run_ends - visits
    positions = jnp.arange(NODE_LIM * TOK_DEV)
    node_of = jnp.sum(positions[:, None] >= run_ends[None, :], axis=1)
    within = positions - run_starts[node_of]
    node_visits = visits[node_of]
    copies = node_visits * PER_VISIT // NODE_EXP
    list_pos = jnp.arange(PER_VISIT)[None, :] * node_visits[:, None] + within[:, None]
    local_rank = list_pos // copies[:, None]
    exp_keys = jax.random.split(key_exp, EP_SIZE)
    exp_perm = jax.vmap(jax.random.permutation)(exp_keys, jnp.tile(jnp.arange(NODE_EXP), (EP_SIZE, 1)))
    expert = node_of[:, None] * NODE_EXP + exp_perm[node_of[:, None], local_rank]
    expert = expert.reshape(NODE_LIM, TOK_DEV, PER_VISIT).transpose(1, 0, 2).reshape(TOK_DEV, TOP_K)
    tok_perm = jax.random.permutation(key_tok, jnp.arange(TOK_DEV))
    return expert[tok_perm].astype(jnp.int32)


def setup_inputs(seed: int = 0, part: int = 0) -> dict:
    part_key = jax.random.fold_in(jax.random.key(seed), part)
    part_keys = jax.random.split(part_key, 4)
    tok_shape = (NUM_SEQ, SEQ_LEN, MODEL_DIM)
    input_a = jax.random.normal(part_keys[0], tok_shape, jnp.float32).astype(jnp.bfloat16)
    input_b = jax.random.normal(part_keys[1], tok_shape, jnp.float32).astype(jnp.bfloat16)
    route_keys = jax.random.split(part_keys[2], 2 * NUM_DEV)
    route_idx = jax.vmap(draw_device_routes)(route_keys).reshape(2, NUM_TOK, TOP_K)
    logits = 0.5 * jax.random.normal(part_keys[3], (2, NUM_TOK, TOP_K), jnp.float32)
    route_gate = TOP_K * jax.nn.softmax(logits, axis=-1)
    w_keys = jax.random.split(jax.random.key(seed + 1), 9)
    proj_shape = (MODEL_DIM, NUM_HEADS, HEAD_DIM)
    attn_norm = jax.random.uniform(w_keys[0], (MODEL_DIM,), jnp.float32, 0.5, 1.5)
    w_query = (jax.random.normal(w_keys[1], proj_shape, jnp.float32) * MODEL_DIM ** -0.5).astype(jnp.bfloat16)
    w_key = (jax.random.normal(w_keys[2], proj_shape, jnp.float32) * MODEL_DIM ** -0.5).astype(jnp.bfloat16)
    w_value = (jax.random.normal(w_keys[3], proj_shape, jnp.float32) * MODEL_DIM ** -0.5).astype(jnp.bfloat16)
    w_out = (jax.random.normal(w_keys[4], (NUM_HEADS, HEAD_DIM, MODEL_DIM), jnp.float32) * (2.0 * (NUM_HEADS * HEAD_DIM) ** -0.5)).astype(jnp.bfloat16)
    moe_norm = jax.random.uniform(w_keys[5], (MODEL_DIM,), jnp.float32, 0.5, 1.5)
    w_gate = (jax.random.normal(w_keys[6], (NUM_EXP, MODEL_DIM, FF_DIM), jnp.float32) * MODEL_DIM ** -0.5).astype(jnp.bfloat16)
    w_up = (jax.random.normal(w_keys[7], (NUM_EXP, MODEL_DIM, FF_DIM), jnp.float32) * MODEL_DIM ** -0.5).astype(jnp.bfloat16)
    w_down = (jax.random.normal(w_keys[8], (NUM_EXP, FF_DIM, MODEL_DIM), jnp.float32) * FF_DIM ** -0.5).astype(jnp.bfloat16)
    return {'input_a': input_a, 'input_b': input_b, 'route_idx': route_idx, 'route_gate': route_gate, 'attn_norm': attn_norm, 'w_query': w_query, 'w_key': w_key, 'w_value': w_value, 'w_out': w_out, 'moe_norm': moe_norm, 'w_gate': w_gate, 'w_up': w_up, 'w_down': w_down}


def rms_norm(values, norm_gain):
    acc_f32 = values.astype(jnp.float32)
    inv_rms = lax.rsqrt(jnp.mean(acc_f32 * acc_f32, axis=-1, keepdims=True) + NORM_EPS)
    return (acc_f32 * inv_rms * norm_gain).astype(jnp.bfloat16)


def attention_seq(seq_tok, attn_norm, w_query, w_key, w_value, w_out):
    normed = rms_norm(seq_tok, attn_norm).astype(jnp.float32)
    q_heads = jnp.einsum('sd,dhc->shc', normed, w_query.astype(jnp.float32)).astype(jnp.bfloat16)
    k_heads = jnp.einsum('sd,dhc->shc', normed, w_key.astype(jnp.float32)).astype(jnp.bfloat16)
    v_heads = jnp.einsum('sd,dhc->shc', normed, w_value.astype(jnp.float32)).astype(jnp.bfloat16)
    scores = jnp.einsum('qhc,khc->hqk', q_heads.astype(jnp.float32), k_heads.astype(jnp.float32)) * HEAD_DIM ** -0.5
    causal = jnp.arange(SEQ_LEN)[:, None] >= jnp.arange(SEQ_LEN)[None, :]
    scores = jnp.where(causal[None, :, :], scores, -jnp.inf)
    prob_bf = jax.nn.softmax(scores, axis=-1).astype(jnp.bfloat16)
    context = jnp.einsum('hqk,khc->qhc', prob_bf.astype(jnp.float32), v_heads.astype(jnp.float32)).astype(jnp.bfloat16)
    proj_out = jnp.einsum('qhc,hcd->qd', context.astype(jnp.float32), w_out.astype(jnp.float32))
    return (seq_tok.astype(jnp.float32) + proj_out).astype(jnp.bfloat16)


def expert_apply(operands):
    expert_rows, gate_mat, up_mat, down_mat = operands
    gate_h = jnp.dot(expert_rows, gate_mat, preferred_element_type=jnp.float32)
    up_h = jnp.dot(expert_rows, up_mat, preferred_element_type=jnp.float32)
    act_rows = (jax.nn.silu(gate_h) * up_h).astype(jnp.bfloat16)
    return jnp.dot(act_rows, down_mat, preferred_element_type=jnp.float32).astype(jnp.bfloat16)


def moe_layer(hidden, exp_ids, gate_w, moe_norm, w_gate, w_up, w_down):
    normed = rms_norm(hidden, moe_norm)
    flat_ids = exp_ids.reshape(-1)
    sort_order = jnp.argsort(flat_ids, stable=True)
    sorted_ids = flat_ids[sort_order]
    counts = jnp.bincount(flat_ids, length=NUM_EXP)
    starts = jnp.cumsum(counts) - counts
    slot_rank = jnp.arange(NUM_TOK * TOP_K) - starts[sorted_ids]
    slot_sorted = sorted_ids * EXP_ROOM + slot_rank
    holder = jnp.full((NUM_EXP * EXP_ROOM,), NUM_TOK, jnp.int32).at[slot_sorted].set(sort_order // TOP_K)
    disp_rows = jnp.take(normed, holder, axis=0, mode='fill', fill_value=0).reshape(NUM_EXP, EXP_ROOM, MODEL_DIM)
    expert_out = lax.map(expert_apply, (disp_rows, w_gate, w_up, w_down))
    slot_of = jnp.zeros_like(flat_ids).at[sort_order].set(slot_sorted)
    picked = jnp.take(expert_out.reshape(NUM_EXP * EXP_ROOM, MODEL_DIM), slot_of, axis=0).reshape(NUM_TOK, TOP_K, MODEL_DIM)
    moe_sum = jnp.sum(gate_w[:, :, None] * picked.astype(jnp.float32), axis=1)
    return (hidden.astype(jnp.float32) + moe_sum).astype(jnp.bfloat16)


def reference(input_a, input_b, route_idx, route_gate, attn_norm, w_query, w_key, w_value, w_out, moe_norm, w_gate, w_up, w_down):
    attend = functools.partial(attention_seq, attn_norm=attn_norm, w_query=w_query, w_key=w_key, w_value=w_value, w_out=w_out)

    def micro_pass(tokens, exp_ids, gate_w):
        hidden = lax.map(attend, tokens).reshape(NUM_TOK, MODEL_DIM)
        mixed_out = moe_layer(hidden, exp_ids, gate_w, moe_norm, w_gate, w_up, w_down)
        return mixed_out.reshape(NUM_SEQ, SEQ_LEN, MODEL_DIM)

    return micro_pass(input_a, route_idx[0], route_gate[0]), micro_pass(input_b, route_idx[1], route_gate[1])
```

```python
import functools

import jax
import jax.numpy as jnp
from jax import lax
from jax.experimental import pallas as pl
from jax.experimental.pallas import tpu as pltpu
from jax.sharding import PartitionSpec as P

NORM_EPS = 1e-6
ROW_TILE = 256
FF_TILE = 256
OUT_TILE = 256
HEADS_STEP = 4
LOG2E = 1.4426950408889634
VMEM_LIMIT = 60 * 1024 * 1024


def rms_norm(values, norm_gain):
    acc_f32 = values.astype(jnp.float32)
    inv_rms = lax.rsqrt(jnp.mean(acc_f32 * acc_f32, axis=-1, keepdims=True) + NORM_EPS)
    return (acc_f32 * inv_rms * norm_gain).astype(jnp.bfloat16)


def attention_kernel(q_ref, k_ref, v_ref, o_ref):
    heads, seq_len, head_dim = q_ref.shape
    half = seq_len // 2
    scale = head_dim ** -0.5 * LOG2E
    lower = lax.broadcasted_iota(jnp.int32, (half, half), 0) >= lax.broadcasted_iota(jnp.int32, (half, half), 1)
    for head in range(heads):
        for part in range(2):
            rows = pl.ds(part * half, half)
            keys = (part + 1) * half
            scores = lax.dot_general(q_ref[head, rows, :], k_ref[head, pl.ds(0, keys), :], (((1,), (1,)), ((), ())), preferred_element_type=jnp.float32)
            diag = jnp.where(lower, scores[:, keys - half:], -jnp.inf)
            top = jnp.max(diag, axis=-1, keepdims=True)
            if part:
                top = jnp.maximum(top, jnp.max(scores[:, :half], axis=-1, keepdims=True))
            expd = jnp.exp2((diag - top) * scale)
            total = jnp.sum(expd, axis=-1, keepdims=True)
            if part:
                exps = jnp.exp2((scores[:, :half] - top) * scale)
                total = total + jnp.sum(exps, axis=-1, keepdims=True)
            inv = 1.0 / total
            ctx = jnp.dot((expd * inv).astype(jnp.bfloat16), v_ref[head, rows, :], preferred_element_type=jnp.float32)
            if part:
                ctx = ctx + jnp.dot((exps * inv).astype(jnp.bfloat16), v_ref[head, pl.ds(0, half), :], preferred_element_type=jnp.float32)
            o_ref[rows, pl.ds(head * head_dim, head_dim)] = ctx.astype(jnp.bfloat16)


def attention_core(q_heads, k_heads, v_heads):
    heads, seq_len, head_dim = q_heads.shape
    spec = pl.BlockSpec((HEADS_STEP, seq_len, head_dim), lambda i: (i, 0, 0))
    return pl.pallas_call(
        attention_kernel,
        grid=(heads // HEADS_STEP,),
        in_specs=[spec] * 3,
        out_specs=pl.BlockSpec((seq_len, HEADS_STEP * head_dim), lambda i: (0, i)),
        out_shape=jax.ShapeDtypeStruct((seq_len, heads * head_dim), jnp.bfloat16),
        compiler_params=pltpu.CompilerParams(dimension_semantics=("arbitrary",)),
        cost_estimate=pl.CostEstimate(flops=25_000_000_000, bytes_accessed=4 * heads * seq_len * head_dim * 2, transcendentals=heads * seq_len * seq_len),
        name="attention_core",
    )(q_heads, k_heads, v_heads)


def attention_block(tokens, attn_norm, w_query, w_key, w_value, w_out, moe_norm):
    seq_len, model_dim = tokens.shape
    normed = rms_norm(tokens, attn_norm)
    q_heads = jnp.einsum('sd,dhc->hsc', normed, w_query, preferred_element_type=jnp.float32).astype(jnp.bfloat16)
    k_heads = jnp.einsum('sd,dhc->hsc', normed, w_key, preferred_element_type=jnp.float32).astype(jnp.bfloat16)
    v_heads = jnp.einsum('sd,dhc->hsc', normed, w_value, preferred_element_type=jnp.float32).astype(jnp.bfloat16)
    context = attention_core(q_heads, k_heads, v_heads)
    proj_out = jnp.dot(context, w_out.reshape(-1, model_dim), preferred_element_type=jnp.float32)
    hidden = (tokens.astype(jnp.float32) + proj_out).astype(jnp.bfloat16)
    return hidden, rms_norm(hidden, moe_norm)


def expert_in_kernel(sources, offs_ref, rank_ref, z_ref, gate_ref, up_ref, u_ref, rows_ref):
    step = pl.program_id(0)
    room = rank_ref.shape[2] * 3 // 4
    toks = rank_ref.shape[2]
    model_dim = z_ref.shape[1]

    @pl.when(step < sources)
    def _():
        base = pl.multiple_of(offs_ref[step], 16)
        pick = (lax.broadcasted_iota(jnp.int32, (room, toks), 0) == rank_ref[0]).astype(jnp.float32).astype(jnp.bfloat16)
        for part in range(4):
            cols = pl.ds(part * (model_dim // 4), model_dim // 4)
            rows_ref[pl.ds(base, room), cols] = jnp.dot(pick, z_ref[:, cols], preferred_element_type=jnp.float32).astype(jnp.bfloat16)

    @pl.when(step == sources - 1)
    def _():
        end = pl.multiple_of(offs_ref[sources], 16)
        rows_ref[pl.ds(end, ROW_TILE), :] = jnp.zeros((ROW_TILE, model_dim), jnp.bfloat16)

    @pl.when(step >= sources)
    def _():
        def tile(index, carry):
            rows = pl.ds(pl.multiple_of(index * ROW_TILE, ROW_TILE), ROW_TILE)
            block = rows_ref[rows, :]
            gate_h = jnp.dot(block, gate_ref[0], preferred_element_type=jnp.float32)
            up_h = jnp.dot(block, up_ref[0], preferred_element_type=jnp.float32)
            u_ref[0, rows, :] = (gate_h * jax.nn.sigmoid(gate_h) * up_h).astype(jnp.bfloat16)
            return carry

        lax.fori_loop(0, (offs_ref[sources] + ROW_TILE - 1) // ROW_TILE, tile, 0)


def expert_in(offs, rank_rows, z_all, w_gate, w_up):
    experts, model_dim, ff_dim = w_gate.shape
    sources, _, toks = rank_rows.shape
    room = sources * toks * 3 // 4
    ff_tiles = ff_dim // FF_TILE

    def weight_map(i, offs_ref):
        j = jnp.maximum(i - sources, 0)
        return (j // ff_tiles, 0, j % ff_tiles)

    return pl.pallas_call(
        functools.partial(expert_in_kernel, sources),
        grid_spec=pltpu.PrefetchScalarGridSpec(
            num_scalar_prefetch=1,
            grid=(sources + experts * ff_tiles,),
            in_specs=[
                pl.BlockSpec((1, 1, toks), lambda i, offs_ref: (jnp.minimum(i, sources - 1), 0, 0)),
                pl.BlockSpec((toks, model_dim), lambda i, offs_ref: (jnp.minimum(i, sources - 1), 0)),
                pl.BlockSpec((1, model_dim, FF_TILE), weight_map),
                pl.BlockSpec((1, model_dim, FF_TILE), weight_map),
            ],
            out_specs=pl.BlockSpec((1, room, FF_TILE), weight_map),
            scratch_shapes=[pltpu.VMEM((room + ROW_TILE, model_dim), jnp.bfloat16)],
        ),
        out_shape=jax.ShapeDtypeStruct((experts, room, ff_dim), jnp.bfloat16),
        compiler_params=pltpu.CompilerParams(dimension_semantics=("arbitrary",), vmem_limit_bytes=VMEM_LIMIT),
        cost_estimate=pl.CostEstimate(flops=130_000_000_000, bytes_accessed=120_000_000, transcendentals=room * ff_dim * experts),
        name="expert_in",
    )(offs, rank_rows, z_all, w_gate, w_up)


def expert_out_kernel(sources, offs_ref, cols_ref, u_ref, down_ref, out_ref, e_ref, place_ref):
    step = pl.program_id(0)
    experts = u_ref.shape[0]
    toks = out_ref.shape[0] // sources
    room = place_ref.shape[2]

    @pl.when(step == 0)
    def _():
        e_ref[...] = jnp.zeros_like(e_ref)
        for source in range(sources):
            rank = cols_ref[pl.ds(source * toks, toks), experts:experts + 1]
            spots = lax.broadcasted_iota(jnp.int32, (toks, room), 1).astype(jnp.float32)
            place_ref[source] = (spots == rank).astype(jnp.float32).astype(jnp.bfloat16)

    def tile(index, carry):
        rows = pl.ds(pl.multiple_of(index * ROW_TILE, ROW_TILE), ROW_TILE)
        for expert in range(experts):
            e_ref[expert, rows, :] = jnp.dot(u_ref[expert, rows, :], down_ref[expert], preferred_element_type=jnp.float32).astype(jnp.bfloat16)
        return carry

    lax.fori_loop(0, (offs_ref[sources] + ROW_TILE - 1) // ROW_TILE, tile, 0)

    def spread(source, carry):
        base = pl.multiple_of(offs_ref[source], 16)
        toks_at = pl.ds(pl.multiple_of(source * toks, toks), toks)
        total = jnp.zeros((toks, out_ref.shape[1]), jnp.float32)
        for expert in range(experts):
            values = jnp.dot(place_ref[source], e_ref[expert, pl.ds(base, room), :], preferred_element_type=jnp.float32)
            total = total + cols_ref[toks_at, expert:expert + 1] * values
        out_ref[toks_at, :] = total
        return carry

    lax.fori_loop(0, sources, spread, 0)


def expert_out(offs, cols, u_rows, w_down):
    experts, ff_dim, model_dim = w_down.shape
    sources = offs.shape[0] - 1
    tok_total = cols.shape[0]
    toks = tok_total // sources
    room = toks * 3 // 4
    return pl.pallas_call(
        functools.partial(expert_out_kernel, sources),
        grid_spec=pltpu.PrefetchScalarGridSpec(
            num_scalar_prefetch=1,
            grid=(model_dim // OUT_TILE,),
            in_specs=[
                pl.BlockSpec((tok_total, cols.shape[1]), lambda i, offs_ref: (0, 0), pipeline_mode=pl.Buffered(1)),
                pl.BlockSpec(u_rows.shape, lambda i, offs_ref: (0, 0, 0), pipeline_mode=pl.Buffered(1)),
                pl.BlockSpec((experts, ff_dim, OUT_TILE), lambda i, offs_ref: (0, 0, i)),
            ],
            out_specs=pl.BlockSpec((tok_total, OUT_TILE), lambda i, offs_ref: (0, i)),
            scratch_shapes=[
                pltpu.VMEM((experts, u_rows.shape[1], OUT_TILE), jnp.bfloat16),
                pltpu.VMEM((sources, toks, room), jnp.bfloat16),
            ],
        ),
        out_shape=jax.ShapeDtypeStruct((tok_total, model_dim), jnp.float32),
        compiler_params=pltpu.CompilerParams(dimension_semantics=("arbitrary",), vmem_limit_bytes=VMEM_LIMIT),
        cost_estimate=pl.CostEstimate(flops=90_000_000_000, bytes_accessed=120_000_000, transcendentals=0),
        name="expert_out",
    )(offs, cols, u_rows, w_down)


def route_tables(route_idx, route_gate, axes, groups, exp_local):
    micro, toks, _ = route_idx.shape
    num_exp = groups * exp_local
    hit = route_idx[:, :, :, None] == jnp.arange(num_exp, dtype=jnp.int32)
    gates = jnp.sum(jnp.where(hit, route_gate[:, :, :, None], 0.0), axis=2)
    seen = jnp.any(hit, axis=2).astype(jnp.float32)
    gates = gates.transpose(2, 0, 1).reshape(groups, exp_local, micro * toks)
    seen = seen.transpose(2, 0, 1).reshape(groups, exp_local, micro * toks)[:, :1]
    table = jnp.concatenate([gates, seen], axis=1).reshape(groups * (exp_local + 1), micro * toks)
    table = lax.all_to_all(table, axes, 0, 0, tiled=True)
    table = table.reshape(groups, exp_local + 1, micro, toks).transpose(2, 0, 1, 3)
    seen = table[:, :, exp_local]
    before = (jnp.arange(toks)[:, None] < jnp.arange(toks)[None, :]).astype(jnp.bfloat16)
    rank = jnp.einsum('mgt,ts->mgs', seen.astype(jnp.bfloat16), before, preferred_element_type=jnp.float32)
    rank = jnp.where(seen > 0, rank, -1.0)
    held = (jnp.sum(seen, axis=-1).astype(jnp.int32) + 15) // 16 * 16
    upto = (jnp.arange(groups + 1)[:, None] > jnp.arange(groups)[None, :]).astype(jnp.int32)
    offs = jnp.sum(held[:, None, :] * upto[None], axis=-1)
    cols = jnp.concatenate([table[:, :, :exp_local], rank[:, :, None]], axis=2).transpose(0, 1, 3, 2).reshape(micro, groups * toks, exp_local + 1)
    return offs, rank.astype(jnp.int32)[:, :, None, :], cols


def solution(mesh):
    axes = ('ep', 'sub')
    groups = mesh.shape['ep'] * mesh.shape['sub']
    tok_spec = P(('dp', 'ep', 'sub'), None, None)
    route_spec = P(None, ('dp', 'ep', 'sub'), None)
    exp_spec = P(('ep', 'sub'), None, None)

    def device_body(input_a, input_b, route_idx, route_gate, attn_norm, w_query, w_key, w_value, w_out, moe_norm, w_gate, w_up, w_down):
        offs, rank_rows, cols = route_tables(route_idx, route_gate, axes, groups, w_gate.shape[0])
        hidden, gathered = [], []
        for tokens in (input_a, input_b):
            h, z = attention_block(tokens[0], attn_norm, w_query, w_key, w_value, w_out, moe_norm)
            hidden.append(h)
            gathered.append(lax.all_gather(z, axes, axis=0, tiled=True))
        outs = []
        for m in range(2):
            u_rows = expert_in(offs[m], rank_rows[m], gathered[m], w_gate, w_up)
            partial = expert_out(offs[m], cols[m], u_rows, w_down)
            moe_sum = lax.psum_scatter(partial, axes, scatter_dimension=0, tiled=True)
            outs.append((hidden[m].astype(jnp.float32) + moe_sum).astype(jnp.bfloat16)[None])
        return tuple(outs)

    return jax.shard_map(device_body, mesh=mesh, in_specs=(tok_spec, tok_spec, route_spec, route_spec, P(), P(), P(), P(), P(), P(), exp_spec, exp_spec, exp_spec), out_specs=(tok_spec, tok_spec), check_vma=False)
```

```python
import functools

import jax
import jax.numpy as jnp
from jax import lax
from jax.experimental import pallas as pl
from jax.experimental.pallas import tpu as pltpu
from jax.sharding import PartitionSpec as P

NORM_EPS = 1e-6
ROW_TILE = 256
FF_TILE = 256
OUT_TILE = 512
CHUNKS = 2
HEADS_STEP = 4
LOG2E = 1.4426950408889634
VMEM_LIMIT = 66_000_000


def rms_norm(values, norm_gain):
    acc_f32 = values.astype(jnp.float32)
    inv_rms = lax.rsqrt(jnp.mean(acc_f32 * acc_f32, axis=-1, keepdims=True) + NORM_EPS)
    return (acc_f32 * inv_rms * norm_gain).astype(jnp.bfloat16)


def attention_kernel(q_ref, k_ref, v_ref, o_ref):
    heads, seq_len, head_dim = q_ref.shape
    half = seq_len // 2
    scale = head_dim ** -0.5 * LOG2E
    lower = lax.broadcasted_iota(jnp.int32, (half, half), 0) >= lax.broadcasted_iota(jnp.int32, (half, half), 1)
    for head in range(heads):
        for part in range(2):
            rows = pl.ds(part * half, half)
            keys = (part + 1) * half
            scores = lax.dot_general(q_ref[head, rows, :], k_ref[head, pl.ds(0, keys), :], (((1,), (1,)), ((), ())), preferred_element_type=jnp.float32)
            diag = jnp.where(lower, scores[:, keys - half:], -jnp.inf)
            top = jnp.max(diag, axis=-1, keepdims=True)
            if part:
                top = jnp.maximum(top, jnp.max(scores[:, :half], axis=-1, keepdims=True))
            expd = jnp.exp2((diag - top) * scale)
            total = jnp.sum(expd, axis=-1, keepdims=True)
            if part:
                exps = jnp.exp2((scores[:, :half] - top) * scale)
                total = total + jnp.sum(exps, axis=-1, keepdims=True)
            inv = 1.0 / total
            ctx = jnp.dot((expd * inv).astype(jnp.bfloat16), v_ref[head, rows, :], preferred_element_type=jnp.float32)
            if part:
                ctx = ctx + jnp.dot((exps * inv).astype(jnp.bfloat16), v_ref[head, pl.ds(0, half), :], preferred_element_type=jnp.float32)
            o_ref[rows, pl.ds(head * head_dim, head_dim)] = ctx.astype(jnp.bfloat16)


def attention_core(q_heads, k_heads, v_heads):
    heads, seq_len, head_dim = q_heads.shape
    spec = pl.BlockSpec((HEADS_STEP, seq_len, head_dim), lambda i: (i, 0, 0))
    return pl.pallas_call(
        attention_kernel,
        grid=(heads // HEADS_STEP,),
        in_specs=[spec] * 3,
        out_specs=pl.BlockSpec((seq_len, HEADS_STEP * head_dim), lambda i: (0, i)),
        out_shape=jax.ShapeDtypeStruct((seq_len, heads * head_dim), jnp.bfloat16),
        compiler_params=pltpu.CompilerParams(dimension_semantics=("arbitrary",)),
        cost_estimate=pl.CostEstimate(flops=25_000_000_000, bytes_accessed=4 * heads * seq_len * head_dim * 2, transcendentals=heads * seq_len * seq_len),
        name="attention_core",
    )(q_heads, k_heads, v_heads)


def after(value, *others):
    return lax.optimization_barrier((value,) + others)[0]


def attention_block(tokens, attn_norm, w_query, w_key, w_value, w_out, moe_norm, ahead=None):
    seq_len, model_dim = tokens.shape
    normed = rms_norm(tokens, attn_norm)
    q_heads = jnp.einsum('sd,dhc->hsc', normed, w_query, preferred_element_type=jnp.float32).astype(jnp.bfloat16)
    k_heads = jnp.einsum('sd,dhc->hsc', normed, w_key, preferred_element_type=jnp.float32).astype(jnp.bfloat16)
    v_heads = jnp.einsum('sd,dhc->hsc', normed, w_value, preferred_element_type=jnp.float32).astype(jnp.bfloat16)
    behind = None
    if ahead is not None:
        q_heads, behind = ahead(q_heads, k_heads, v_heads)
    context = attention_core(q_heads, k_heads, v_heads)
    if behind is not None:
        context = after(context, *behind)
    proj_out = jnp.dot(context, w_out.reshape(-1, model_dim), preferred_element_type=jnp.float32)
    hidden = (tokens.astype(jnp.float32) + proj_out).astype(jnp.bfloat16)
    return hidden, rms_norm(hidden, moe_norm)


def row_tiles(count, run):
    tiles = (count + ROW_TILE - 1) // ROW_TILE

    def pair(index, carry):
        run(pl.multiple_of(index * (2 * ROW_TILE), 2 * ROW_TILE), 2 * ROW_TILE)
        return carry

    lax.fori_loop(0, tiles // 2, pair, 0)

    @pl.when(tiles % 2 == 1)
    def _():
        run(pl.multiple_of((tiles - 1) * ROW_TILE, ROW_TILE), ROW_TILE)


def expert_in_kernel(nodes, room, offs_ref, rank_ref, *refs):
    z_parts, weights, (u_ref, rows_ref, z_ref, z_sem) = refs[:8], refs[8:-4], refs[-4:]
    step = pl.program_id(0)
    half, model_dim = z_parts[0].shape
    toks = 2 * half
    sources = 4
    ends = sources + 1
    node_room = sources * room
    per_node = (pl.num_programs(0) - 1) // len(nodes)

    @pl.when(step == 0)
    def _():
        def copies(source):
            slot = source % 2
            return [pltpu.make_async_copy(z_parts[2 * source + n], z_ref.at[slot, pl.ds(n * half, half)], z_sem.at[slot, n]) for n in range(2)]

        for copy in copies(0):
            copy.start()
        for at, node in enumerate(nodes):
            end = pl.multiple_of(offs_ref[node * ends + sources] + at * node_room, 16)
            rows_ref[pl.ds(end, ROW_TILE), :] = jnp.zeros((ROW_TILE, model_dim), jnp.bfloat16)
        for source in range(sources):
            if source + 1 < sources:
                for copy in copies(source + 1):
                    copy.start()
            for copy in copies(source):
                copy.wait()
            for at, node in enumerate(nodes):
                base = pl.multiple_of(offs_ref[node * ends + source] + at * node_room, 16)
                pick = (lax.broadcasted_iota(jnp.int32, (room, toks), 0) == rank_ref[node * sources + source]).astype(jnp.float32).astype(jnp.bfloat16)
                for part in range(4):
                    cols = pl.ds(part * (model_dim // 4), model_dim // 4)
                    rows_ref[pl.ds(base, room), cols] = jnp.dot(pick, z_ref[source % 2, :, cols], preferred_element_type=jnp.float32).astype(jnp.bfloat16)

    for at, node in enumerate(nodes):
        gate_ref, up_ref = weights[2 * at], weights[2 * at + 1]

        @pl.when((step > at * per_node) & (step <= (at + 1) * per_node))
        def _():
            def run(start, size):
                block = rows_ref[pl.ds(at * node_room + start, size), :]
                gate_h = jnp.dot(block, gate_ref[0], preferred_element_type=jnp.float32)
                up_h = jnp.dot(block, up_ref[0], preferred_element_type=jnp.float32)
                u_ref[0, pl.ds(start, size), :] = (gate_h * jax.nn.sigmoid(gate_h) * up_h).astype(jnp.bfloat16)

            row_tiles(offs_ref[node * ends + sources], run)


def expert_in(nodes, offs, rank_rows, z_parts, weights):
    experts, model_dim, ff_dim = weights[0].shape
    groups, _, toks = rank_rows.shape
    room = toks * 3 // 4
    ff_tiles = ff_dim // FF_TILE
    per_node = experts * ff_tiles

    def weight_map(first):
        def index(i, offs_ref):
            j = jnp.clip(i - first, 0, per_node - 1)
            return (j // ff_tiles, 0, j % ff_tiles)

        return index

    def u_map(i, offs_ref):
        j = jnp.maximum(i - 1, 0)
        return (j // ff_tiles, 0, j % ff_tiles)

    rows = groups // 2 * room
    return pl.pallas_call(
        functools.partial(expert_in_kernel, nodes, room),
        grid_spec=pltpu.PrefetchScalarGridSpec(
            num_scalar_prefetch=1,
            grid=(1 + len(nodes) * per_node,),
            in_specs=[pl.BlockSpec(rank_rows.shape, lambda i, offs_ref: (0, 0, 0), pipeline_mode=pl.Buffered(1))]
            + [pl.BlockSpec(memory_space=pl.ANY)] * 8
            + [pl.BlockSpec((1, model_dim, FF_TILE), weight_map(1 + n // 2 * per_node)) for n in range(2 * len(nodes))],
            out_specs=pl.BlockSpec((1, rows, FF_TILE), u_map),
            scratch_shapes=[
                pltpu.VMEM((len(nodes) * rows + ROW_TILE, model_dim), jnp.bfloat16),
                pltpu.VMEM((2, toks, model_dim), jnp.bfloat16),
                pltpu.SemaphoreType.DMA((2, 2)),
            ],
        ),
        out_shape=jax.ShapeDtypeStruct((len(nodes) * experts, rows, ff_dim), jnp.bfloat16),
        compiler_params=pltpu.CompilerParams(dimension_semantics=("arbitrary",), vmem_limit_bytes=VMEM_LIMIT),
        cost_estimate=pl.CostEstimate(flops=65_000_000_000 * len(nodes), bytes_accessed=75_000_000 * len(nodes), transcendentals=0),
        name="expert_in",
    )(offs, rank_rows, *z_parts, *weights)


def expert_out_kernel(offs_ref, cols_ref, down_a, down_b, *refs):
    u_parts, (send_x, keep_x, send_y, keep_y, u_ref, e_ref, place_ref, sum_ref, u_sem) = refs[:-9], refs[-9:]
    step = pl.program_id(0)
    experts = u_ref.shape[0]
    whole = [part.at[n] for part in u_parts for n in range(part.shape[0])]
    loads = [pltpu.make_async_copy(part, u_ref.at[n], u_sem.at[n]) for n, part in enumerate(whole)]
    per_node = experts // 2
    sources, toks, room = place_ref.shape[0] // 2, place_ref.shape[1], place_ref.shape[2]
    ends = sources + 1

    @pl.when(step == 0)
    def _():
        for load in loads:
            load.start()
        e_ref[...] = jnp.zeros_like(e_ref)
        for node in range(2):
            for source in range(sources):
                rank = cols_ref[pl.ds(source * toks, toks), experts + node:experts + node + 1]
                spots = lax.broadcasted_iota(jnp.int32, (toks, room), 1).astype(jnp.float32)
                place_ref[node * sources + source] = (spots == rank).astype(jnp.float32).astype(jnp.bfloat16)

    for expert in range(experts):
        @pl.when(step == 0)
        def _():
            loads[expert].wait()

        def run(start, size):
            down = (down_a, down_b)[expert // per_node]
            e_ref[expert, pl.ds(start, size), :] = jnp.dot(u_ref[expert, pl.ds(start, size), :], down[expert % per_node], preferred_element_type=jnp.float32).astype(jnp.bfloat16)

        row_tiles(offs_ref[expert // per_node * ends + sources], run)

    def spread(source, carry):
        toks_at = pl.ds(pl.multiple_of(source * toks, toks), toks)
        total = None
        for node in range(2):
            base = pl.multiple_of(offs_ref[node * ends + source], 16)
            for local in range(per_node):
                expert = node * per_node + local
                values = jnp.dot(place_ref[node * sources + source], e_ref[expert, pl.ds(base, room), :], preferred_element_type=jnp.float32)
                values = cols_ref[toks_at, expert:expert + 1] * values
                total = values if total is None else total + values
        sum_ref[source] = total
        return carry

    lax.fori_loop(0, sources, spread, 0)

    @pl.when(step < pl.num_programs(0) // 2)
    def _():
        send_x[0] = sum_ref[1]
        send_x[1] = sum_ref[3]
        keep_x[0] = sum_ref[0]
        keep_x[1] = sum_ref[2]

    @pl.when(step >= pl.num_programs(0) // 2)
    def _():
        send_y[0] = sum_ref[2]
        send_y[1] = sum_ref[3]
        keep_y[0] = sum_ref[0]
        keep_y[1] = sum_ref[1]


def expert_out(chunk, offs, cols, u_parts, own, peer):
    experts, ff_dim, model_dim = own.shape
    toks = cols.shape[0] // 4
    room = toks * 3 // 4
    width = model_dim // CHUNKS
    steps = width // OUT_TILE
    half = steps // 2
    weight = pl.BlockSpec((experts, ff_dim, OUT_TILE), lambda i, offs_ref: (0, 0, chunk * steps + i))
    out_x = pl.BlockSpec((2, toks, OUT_TILE), lambda i, offs_ref: (0, 0, jnp.minimum(i, half - 1)))
    out_y = pl.BlockSpec((2, toks, OUT_TILE), lambda i, offs_ref: (0, 0, jnp.maximum(i - half, 0)))
    return pl.pallas_call(
        expert_out_kernel,
        grid_spec=pltpu.PrefetchScalarGridSpec(
            num_scalar_prefetch=1,
            grid=(steps,),
            in_specs=[
                pl.BlockSpec(cols.shape, lambda i, offs_ref: (0, 0), pipeline_mode=pl.Buffered(1)),
                weight,
                weight,
            ] + [pl.BlockSpec(memory_space=pl.ANY)] * len(u_parts),
            out_specs=[out_x, out_x, out_y, out_y],
            scratch_shapes=[
                pltpu.VMEM((2 * experts, 4 * room, ff_dim), jnp.bfloat16),
                pltpu.VMEM((2 * experts, 4 * room, OUT_TILE), jnp.bfloat16),
                pltpu.VMEM((8, toks, room), jnp.bfloat16),
                pltpu.VMEM((4, toks, OUT_TILE), jnp.float32),
                pltpu.SemaphoreType.DMA((2 * experts,)),
            ],
        ),
        out_shape=[jax.ShapeDtypeStruct((2, toks, width // 2), jnp.float32)] * 4,
        compiler_params=pltpu.CompilerParams(dimension_semantics=("arbitrary",), vmem_limit_bytes=VMEM_LIMIT),
        cost_estimate=pl.CostEstimate(flops=90_000_000_000 // CHUNKS, bytes_accessed=70_000_000, transcendentals=0),
        name="expert_out",
    )(offs, cols, own, peer, *u_parts)


def to_x(values):
    return lax.ppermute(values, 'ep', [(0, 2), (1, 3), (2, 0), (3, 1)])


def to_y(values):
    return lax.ppermute(values, 'sub', [(0, 1), (1, 0)])


def to_core(values):
    return lax.ppermute(values, 'ep', [(0, 1), (1, 0), (2, 3), (3, 2)])


def local_table(route_idx, route_gate, ep_size, node_exp):
    micro, toks, _ = route_idx.shape
    num_exp = ep_size * node_exp
    hit = route_idx[:, :, :, None] == jnp.arange(num_exp, dtype=jnp.int32)
    gates = jnp.sum(jnp.where(hit, route_gate[:, :, :, None], 0.0), axis=2)
    seen = jnp.any((route_idx // node_exp)[:, :, :, None] == jnp.arange(ep_size, dtype=jnp.int32), axis=2)
    return jnp.concatenate([gates, seen.astype(jnp.float32)], axis=2).transpose(2, 0, 1).reshape(num_exp + ep_size, micro * toks)


def route_tables(table, micro, toks, ep_size, sub_size, exp_local):
    room = toks * 3 // 4
    num_exp = ep_size * sub_size * exp_local
    table_y = to_y(table)
    tables = jnp.stack([table, to_x(table), table_y, to_x(table_y)])
    node, sub = lax.axis_index('ep'), lax.axis_index('sub')
    peer = node ^ 1
    take = lambda first, size: lax.dynamic_slice_in_dim(tables, first, size, axis=1)
    gates = jnp.concatenate([take((n * sub_size + sub) * exp_local, exp_local) for n in (node, peer)], axis=1)
    seen = jnp.concatenate([take(num_exp + n, 1) for n in (node, peer)], axis=1)
    gates = gates.reshape(4, 2 * exp_local, micro, toks).transpose(2, 0, 3, 1)
    seen = seen.reshape(4, 2, micro, toks).transpose(2, 1, 0, 3)
    before = (jnp.arange(toks)[:, None] < jnp.arange(toks)[None, :]).astype(jnp.bfloat16)
    rank = jnp.einsum('mnst,tu->mnsu', seen.astype(jnp.bfloat16), before, preferred_element_type=jnp.float32)
    rank = jnp.where(seen > 0, rank, -1.0)
    held = (jnp.sum(seen, axis=-1).astype(jnp.int32) + 15) // 16 * 16
    upto = (jnp.arange(5)[:, None] > jnp.arange(4)[None, :]).astype(jnp.int32)
    offs = jnp.sum(held[:, :, None, :] * upto, axis=-1)
    cols = jnp.concatenate([gates, rank.transpose(0, 2, 3, 1)], axis=3).reshape(micro, 4 * toks, 2 * exp_local + 2)
    return offs.reshape(micro, 10), rank.astype(jnp.int32).reshape(micro, 8, 1, toks), cols


def solution(mesh):
    ep_size = mesh.shape['ep']
    sub_size = mesh.shape['sub']
    tok_spec = P(('dp', 'ep', 'sub'), None, None)
    route_spec = P(None, ('dp', 'ep', 'sub'), None)
    exp_spec = P(('ep', 'sub'), None, None)

    def device_body(input_a, input_b, route_idx, route_gate, attn_norm, w_query, w_key, w_value, w_out, moe_norm, w_gate, w_up, w_down):
        micro, toks, _ = route_idx.shape
        table = local_table(route_idx, route_gate, ep_size, sub_size * w_gate.shape[0])
        offs, rank_rows, cols = route_tables(table, micro, toks, ep_size, sub_size, w_gate.shape[0])
        peer_gate, peer_up, peer_down = to_core(w_gate), to_core(w_up), to_core(w_down)
        attend = functools.partial(attention_block, attn_norm=attn_norm, w_query=w_query, w_key=w_key, w_value=w_value, w_out=w_out, moe_norm=moe_norm)

        def gather_near(z):
            top, bot = z[:toks // 2], z[toks // 2:]
            y_top, x_bot = to_y(top), to_x(bot)
            return top, bot, to_x(top), x_bot, y_top, to_y(bot)

        def gather_far(near, *others):
            y_top, x_bot = lax.optimization_barrier((near[4], near[3]) + others)[:2]
            return near + (to_x(y_top), to_y(x_bot))

        weights = ((w_gate, w_up), (peer_gate, peer_up))

        def experts_in(m, nodes, starts, parts):
            return expert_in(nodes, starts, rank_rows[m], parts, sum((weights[n] for n in nodes), ()))

        def experts_out(m, chunk, starts, *u_parts):
            send_x, keep_x, send_y, keep_y = expert_out(chunk, starts, cols[m], u_parts, w_down, peer_down)
            return keep_x, keep_y, to_x(send_x), to_y(send_y), send_x

        def forward(sent):
            keep_x, keep_y, got_x, got_y, _ = sent
            return keep_x[1] + got_x[1], keep_y[1] + got_y[1]

        def arrive(forwards):
            rest_x, rest_y = forwards
            return to_y(rest_x), to_x(rest_y)

        def finish(hidden, sents, arrived):
            pieces = []
            for (keep_x, keep_y, got_x, got_y, _), (rest_x, rest_y) in zip(sents, arrived):
                pieces.append((keep_x[0] + got_x[0]) + rest_x)
                pieces.append((keep_y[0] + got_y[0]) + rest_y)
            width = pieces[0].shape[1]
            done = [(hidden[:, n * width:(n + 1) * width].astype(jnp.float32) + piece).astype(jnp.bfloat16) for n, piece in enumerate(pieces)]
            return jnp.concatenate(done, axis=1)[None]

        hidden_a, z_a = attend(after(input_a[0], table))
        near_a = gather_near(z_a)
        parts_a = []

        def far_of_a(q_heads, k_heads, v_heads):
            parts_a.append(gather_far(near_a, q_heads, k_heads, v_heads))
            return after(q_heads, near_a[4], near_a[3]), parts_a[0][6:]

        hidden_b, z_b = attend(after(input_b[0], z_a, offs, rank_rows, cols), ahead=far_of_a)
        near_b = gather_near(z_b)
        starts_a = after(offs[0], z_b)
        u_a = experts_in(0, (0, 1), starts_a, parts_a[0])
        parts_b = gather_far(near_b, u_a)
        starts_a0 = after(starts_a, u_a, near_b[4], near_b[3])
        sent_a0 = experts_out(0, 0, starts_a0, u_a)
        sent_a1 = experts_out(0, 1, after(starts_a0, sent_a0[-1], *parts_b[6:]), u_a)
        starts_b = after(offs[1], sent_a1[-1])
        u_b0 = experts_in(1, (0,), starts_b, parts_b)
        forward_a0 = forward(sent_a0)
        starts_b = after(starts_b, u_b0, *forward_a0)
        u_b1 = experts_in(1, (1,), starts_b, parts_b)
        forward_a1 = forward(sent_a1)
        arrived_a0 = arrive(forward_a0)
        starts_b = after(starts_b, u_b1, *forward_a1, *arrived_a0)
        sent_b0 = experts_out(1, 0, starts_b, u_b0, u_b1)
        arrived_a1 = arrive(forward_a1)
        starts_b = after(starts_b, sent_b0[-1], *arrived_a1)
        sent_b1 = experts_out(1, 1, starts_b, u_b0, u_b1)
        arrived_b = [arrive(forward(sent_b0)), arrive(forward(sent_b1))]
        return finish(hidden_a, [sent_a0, sent_a1], [arrived_a0, arrived_a1]), finish(hidden_b, [sent_b0, sent_b1], arrived_b)

    return jax.shard_map(device_body, mesh=mesh, in_specs=(tok_spec, tok_spec, route_spec, route_spec, P(), P(), P(), P(), P(), P(), exp_spec, exp_spec, exp_spec), out_specs=(tok_spec, tok_spec), check_vma=False)
```

```python
import functools

import jax
import jax.numpy as jnp
from jax import lax
from jax.experimental import pallas as pl
from jax.experimental.pallas import tpu as pltpu
from jax.sharding import PartitionSpec as P

NORM_EPS = 1e-6
ROW_TILE = 256
FF_TILE = 256
OUT_TILE = 512
CHUNKS = 2
HEADS_STEP = 8
LOG2E = 1.4426950408889634
VMEM_LIMIT = 66_000_000


def rms_norm(values, norm_gain):
    acc_f32 = values.astype(jnp.float32)
    inv_rms = lax.rsqrt(jnp.mean(acc_f32 * acc_f32, axis=-1, keepdims=True) + NORM_EPS)
    return (acc_f32 * inv_rms * norm_gain).astype(jnp.bfloat16)


def attention_kernel(q_ref, k_ref, v_ref, o_ref):
    heads, seq_len, head_dim = q_ref.shape
    half = seq_len // 2
    scale = head_dim ** -0.5 * LOG2E
    lower = lax.broadcasted_iota(jnp.int32, (half, half), 0) >= lax.broadcasted_iota(jnp.int32, (half, half), 1)
    units = [(head, part) for head in range(heads) for part in range(2)]

    def score(head, part):
        return lax.dot_general(q_ref[head, pl.ds(part * half, half), :], k_ref[head, pl.ds(0, (part + 1) * half), :], (((1,), (1,)), ((), ())), preferred_element_type=jnp.float32)

    def emit(head, part, probs):
        ctx = jnp.dot(probs, v_ref[head, pl.ds(0, (part + 1) * half), :], preferred_element_type=jnp.float32)
        o_ref[pl.ds(part * half, half), pl.ds(head * head_dim, head_dim)] = ctx.astype(jnp.bfloat16)

    ahead, behind = score(*units[0]), None
    for index, (head, part) in enumerate(units):
        scores = ahead
        if index + 1 < len(units):
            ahead = score(*units[index + 1])
        if behind is not None:
            emit(*behind)
        masked = jnp.where(lower, scores[:, part * half:], -jnp.inf)
        if part:
            masked = jnp.concatenate([scores[:, :half], masked], axis=1)
        expd = jnp.exp2((masked - jnp.max(masked, axis=-1, keepdims=True)) * scale)
        inv = 1.0 / jnp.sum(expd, axis=-1, keepdims=True)
        behind = (head, part, (expd * inv).astype(jnp.bfloat16))
    emit(*behind)


def attention_core(q_heads, k_heads, v_heads):
    heads, seq_len, head_dim = q_heads.shape
    spec = pl.BlockSpec((HEADS_STEP, seq_len, head_dim), lambda i: (i, 0, 0))
    return pl.pallas_call(
        attention_kernel,
        grid=(heads // HEADS_STEP,),
        in_specs=[spec] * 3,
        out_specs=pl.BlockSpec((seq_len, HEADS_STEP * head_dim), lambda i: (0, i)),
        out_shape=jax.ShapeDtypeStruct((seq_len, heads * head_dim), jnp.bfloat16),
        compiler_params=pltpu.CompilerParams(dimension_semantics=("arbitrary",)),
        cost_estimate=pl.CostEstimate(flops=25_000_000_000, bytes_accessed=4 * heads * seq_len * head_dim * 2, transcendentals=heads * seq_len * seq_len),
        name="attention_core",
    )(q_heads, k_heads, v_heads)


def after(value, *others):
    return lax.optimization_barrier((value,) + others)[0]


def attention_block(tokens, attn_norm, w_query, w_key, w_value, w_out, moe_norm, ahead=None):
    seq_len, model_dim = tokens.shape
    normed = rms_norm(tokens, attn_norm)
    q_heads = jnp.einsum('sd,dhc->hsc', normed, w_query, preferred_element_type=jnp.float32).astype(jnp.bfloat16)
    k_heads = jnp.einsum('sd,dhc->hsc', normed, w_key, preferred_element_type=jnp.float32).astype(jnp.bfloat16)
    v_heads = jnp.einsum('sd,dhc->hsc', normed, w_value, preferred_element_type=jnp.float32).astype(jnp.bfloat16)
    behind = None
    if ahead is not None:
        q_heads, behind = ahead(q_heads, k_heads, v_heads)
    context = attention_core(q_heads, k_heads, v_heads)
    if behind is not None:
        context = after(context, *behind)
    proj_out = jnp.dot(context, w_out.reshape(-1, model_dim), preferred_element_type=jnp.float32)
    hidden = (tokens.astype(jnp.float32) + proj_out).astype(jnp.bfloat16)
    return hidden, rms_norm(hidden, moe_norm)


def row_tiles(count, run):
    tiles = (count + ROW_TILE - 1) // ROW_TILE

    def pair(index, carry):
        run(pl.multiple_of(index * (2 * ROW_TILE), 2 * ROW_TILE), 2 * ROW_TILE)
        return carry

    lax.fori_loop(0, tiles // 2, pair, 0)

    @pl.when(tiles % 2 == 1)
    def _():
        run(pl.multiple_of((tiles - 1) * ROW_TILE, ROW_TILE), ROW_TILE)


def expert_in_kernel(nodes, room, offs_ref, rank_ref, *refs):
    z_parts, weights, (u_ref, rows_ref, z_ref, z_sem) = refs[:8], refs[8:-4], refs[-4:]
    step = pl.program_id(0)
    half, model_dim = z_parts[0].shape
    toks = 2 * half
    sources = 4
    ends = sources + 1
    node_room = sources * room
    per_node = (pl.num_programs(0) - 1) // len(nodes)

    @pl.when(step == 0)
    def _():
        def copies(source):
            slot = source % 2
            return [pltpu.make_async_copy(z_parts[2 * source + n], z_ref.at[slot, pl.ds(n * half, half)], z_sem.at[slot, n]) for n in range(2)]

        for copy in copies(0):
            copy.start()
        for at, node in enumerate(nodes):
            end = pl.multiple_of(offs_ref[node * ends + sources] + at * node_room, 16)
            rows_ref[pl.ds(end, ROW_TILE), :] = jnp.zeros((ROW_TILE, model_dim), jnp.bfloat16)
        for source in range(sources):
            if source + 1 < sources:
                for copy in copies(source + 1):
                    copy.start()
            for copy in copies(source):
                copy.wait()
            for at, node in enumerate(nodes):
                base = pl.multiple_of(offs_ref[node * ends + source] + at * node_room, 16)
                pick = (lax.broadcasted_iota(jnp.int32, (room, toks), 0) == rank_ref[node * sources + source]).astype(jnp.float32).astype(jnp.bfloat16)
                for part in range(4):
                    cols = pl.ds(part * (model_dim // 4), model_dim // 4)
                    rows_ref[pl.ds(base, room), cols] = jnp.dot(pick, z_ref[source % 2, :, cols], preferred_element_type=jnp.float32).astype(jnp.bfloat16)

    for at, node in enumerate(nodes):
        gate_ref, up_ref = weights[2 * at], weights[2 * at + 1]

        @pl.when((step > at * per_node) & (step <= (at + 1) * per_node))
        def _():
            def run(start, size):
                block = rows_ref[pl.ds(at * node_room + start, size), :]
                gate_h = jnp.dot(block, gate_ref[0], preferred_element_type=jnp.float32)
                up_h = jnp.dot(block, up_ref[0], preferred_element_type=jnp.float32)
                u_ref[0, pl.ds(start, size), :] = (gate_h * jax.nn.sigmoid(gate_h) * up_h).astype(jnp.bfloat16)

            row_tiles(offs_ref[node * ends + sources], run)


def expert_in(nodes, offs, rank_rows, z_parts, weights):
    experts, model_dim, ff_dim = weights[0].shape
    groups, _, toks = rank_rows.shape
    room = toks * 3 // 4
    ff_tiles = ff_dim // FF_TILE
    per_node = experts * ff_tiles

    def weight_map(first):
        def index(i, offs_ref):
            j = jnp.clip(i - first, 0, per_node - 1)
            return (j // ff_tiles, 0, j % ff_tiles)

        return index

    def u_map(i, offs_ref):
        j = jnp.maximum(i - 1, 0)
        return (j // ff_tiles, 0, j % ff_tiles)

    rows = groups // 2 * room
    return pl.pallas_call(
        functools.partial(expert_in_kernel, nodes, room),
        grid_spec=pltpu.PrefetchScalarGridSpec(
            num_scalar_prefetch=1,
            grid=(1 + len(nodes) * per_node,),
            in_specs=[pl.BlockSpec(rank_rows.shape, lambda i, offs_ref: (0, 0, 0), pipeline_mode=pl.Buffered(1))]
            + [pl.BlockSpec(memory_space=pl.ANY)] * 8
            + [pl.BlockSpec((1, model_dim, FF_TILE), weight_map(1 + n // 2 * per_node)) for n in range(2 * len(nodes))],
            out_specs=pl.BlockSpec((1, rows, FF_TILE), u_map),
            scratch_shapes=[
                pltpu.VMEM((len(nodes) * rows + ROW_TILE, model_dim), jnp.bfloat16),
                pltpu.VMEM((2, toks, model_dim), jnp.bfloat16),
                pltpu.SemaphoreType.DMA((2, 2)),
            ],
        ),
        out_shape=jax.ShapeDtypeStruct((len(nodes) * experts, rows, ff_dim), jnp.bfloat16),
        compiler_params=pltpu.CompilerParams(dimension_semantics=("arbitrary",), vmem_limit_bytes=VMEM_LIMIT),
        cost_estimate=pl.CostEstimate(flops=65_000_000_000 * len(nodes), bytes_accessed=75_000_000 * len(nodes), transcendentals=0),
        name="expert_in",
    )(offs, rank_rows, *z_parts, *weights)


def expert_out_kernel(offs_ref, cols_ref, down_a, down_b, *refs):
    u_parts, (send_x, keep_x, send_y, keep_y, u_ref, e_ref, place_ref, sum_ref, u_sem) = refs[:-9], refs[-9:]
    step = pl.program_id(0)
    experts = u_ref.shape[0]
    whole = [part.at[n] for part in u_parts for n in range(part.shape[0])]
    loads = [pltpu.make_async_copy(part, u_ref.at[n], u_sem.at[n]) for n, part in enumerate(whole)]
    per_node = experts // 2
    sources, toks, room = place_ref.shape[0] // 2, place_ref.shape[1], place_ref.shape[2]
    ends = sources + 1

    @pl.when(step == 0)
    def _():
        for load in loads:
            load.start()
        e_ref[...] = jnp.zeros_like(e_ref)
        for node in range(2):
            for source in range(sources):
                rank = cols_ref[pl.ds(source * toks, toks), experts + node:experts + node + 1]
                spots = lax.broadcasted_iota(jnp.int32, (toks, room), 1).astype(jnp.float32)
                place_ref[node * sources + source] = (spots == rank).astype(jnp.float32).astype(jnp.bfloat16)

    for expert in range(experts):
        @pl.when(step == 0)
        def _():
            loads[expert].wait()

        def run(start, size):
            down = (down_a, down_b)[expert // per_node]
            e_ref[expert, pl.ds(start, size), :] = jnp.dot(u_ref[expert, pl.ds(start, size), :], down[expert % per_node], preferred_element_type=jnp.float32).astype(jnp.bfloat16)

        row_tiles(offs_ref[expert // per_node * ends + sources], run)

    def spread(source, carry):
        toks_at = pl.ds(pl.multiple_of(source * toks, toks), toks)
        total = None
        for node in range(2):
            base = pl.multiple_of(offs_ref[node * ends + source], 16)
            for local in range(per_node):
                expert = node * per_node + local
                values = jnp.dot(place_ref[node * sources + source], e_ref[expert, pl.ds(base, room), :], preferred_element_type=jnp.float32)
                values = cols_ref[toks_at, expert:expert + 1] * values
                total = values if total is None else total + values
        sum_ref[source] = total
        return carry

    lax.fori_loop(0, sources, spread, 0)

    @pl.when(step < pl.num_programs(0) // 2)
    def _():
        send_x[0] = sum_ref[1]
        send_x[1] = sum_ref[3]
        keep_x[0] = sum_ref[0]
        keep_x[1] = sum_ref[2]

    @pl.when(step >= pl.num_programs(0) // 2)
    def _():
        send_y[0] = sum_ref[2]
        send_y[1] = sum_ref[3]
        keep_y[0] = sum_ref[0]
        keep_y[1] = sum_ref[1]


def expert_out(chunk, offs, cols, u_parts, own, peer):
    experts, ff_dim, model_dim = own.shape
    toks = cols.shape[0] // 4
    room = toks * 3 // 4
    width = model_dim // CHUNKS
    steps = width // OUT_TILE
    half = steps // 2
    weight = pl.BlockSpec((experts, ff_dim, OUT_TILE), lambda i, offs_ref: (0, 0, chunk * steps + i))
    out_x = pl.BlockSpec((2, toks, OUT_TILE), lambda i, offs_ref: (0, 0, jnp.minimum(i, half - 1)))
    out_y = pl.BlockSpec((2, toks, OUT_TILE), lambda i, offs_ref: (0, 0, jnp.maximum(i - half, 0)))
    return pl.pallas_call(
        expert_out_kernel,
        grid_spec=pltpu.PrefetchScalarGridSpec(
            num_scalar_prefetch=1,
            grid=(steps,),
            in_specs=[
                pl.BlockSpec(cols.shape, lambda i, offs_ref: (0, 0), pipeline_mode=pl.Buffered(1)),
                weight,
                weight,
            ] + [pl.BlockSpec(memory_space=pl.ANY)] * len(u_parts),
            out_specs=[out_x, out_x, out_y, out_y],
            scratch_shapes=[
                pltpu.VMEM((2 * experts, 4 * room, ff_dim), jnp.bfloat16),
                pltpu.VMEM((2 * experts, 4 * room, OUT_TILE), jnp.bfloat16),
                pltpu.VMEM((8, toks, room), jnp.bfloat16),
                pltpu.VMEM((4, toks, OUT_TILE), jnp.float32),
                pltpu.SemaphoreType.DMA((2 * experts,)),
            ],
        ),
        out_shape=[jax.ShapeDtypeStruct((2, toks, width // 2), jnp.float32)] * 4,
        compiler_params=pltpu.CompilerParams(dimension_semantics=("arbitrary",), vmem_limit_bytes=VMEM_LIMIT),
        cost_estimate=pl.CostEstimate(flops=90_000_000_000 // CHUNKS, bytes_accessed=70_000_000, transcendentals=0),
        name="expert_out",
    )(offs, cols, own, peer, *u_parts)


def to_x(values):
    return lax.ppermute(values, 'ep', [(0, 2), (1, 3), (2, 0), (3, 1)])


def to_y(values):
    return lax.ppermute(values, 'sub', [(0, 1), (1, 0)])


def to_core(values):
    return lax.ppermute(values, 'ep', [(0, 1), (1, 0), (2, 3), (3, 2)])


def local_table(route_idx, route_gate, ep_size, node_exp):
    micro, toks, _ = route_idx.shape
    num_exp = ep_size * node_exp
    hit = route_idx[:, :, :, None] == jnp.arange(num_exp, dtype=jnp.int32)
    gates = jnp.sum(jnp.where(hit, route_gate[:, :, :, None], 0.0), axis=2)
    seen = jnp.any((route_idx // node_exp)[:, :, :, None] == jnp.arange(ep_size, dtype=jnp.int32), axis=2)
    return jnp.concatenate([gates, seen.astype(jnp.float32)], axis=2).transpose(2, 0, 1).reshape(num_exp + ep_size, micro * toks)


def route_tables(table, micro, toks, ep_size, sub_size, exp_local):
    room = toks * 3 // 4
    num_exp = ep_size * sub_size * exp_local
    table_y = to_y(table)
    tables = jnp.stack([table, to_x(table), table_y, to_x(table_y)])
    node, sub = lax.axis_index('ep'), lax.axis_index('sub')
    peer = node ^ 1
    take = lambda first, size: lax.dynamic_slice_in_dim(tables, first, size, axis=1)
    gates = jnp.concatenate([take((n * sub_size + sub) * exp_local, exp_local) for n in (node, peer)], axis=1)
    seen = jnp.concatenate([take(num_exp + n, 1) for n in (node, peer)], axis=1)
    gates = gates.reshape(4, 2 * exp_local, micro, toks).transpose(2, 0, 3, 1)
    seen = seen.reshape(4, 2, micro, toks).transpose(2, 1, 0, 3)
    before = (jnp.arange(toks)[:, None] < jnp.arange(toks)[None, :]).astype(jnp.bfloat16)
    rank = jnp.einsum('mnst,tu->mnsu', seen.astype(jnp.bfloat16), before, preferred_element_type=jnp.float32)
    rank = jnp.where(seen > 0, rank, -1.0)
    held = (jnp.sum(seen, axis=-1).astype(jnp.int32) + 15) // 16 * 16
    upto = (jnp.arange(5)[:, None] > jnp.arange(4)[None, :]).astype(jnp.int32)
    offs = jnp.sum(held[:, :, None, :] * upto, axis=-1)
    cols = jnp.concatenate([gates, rank.transpose(0, 2, 3, 1)], axis=3).reshape(micro, 4 * toks, 2 * exp_local + 2)
    return offs.reshape(micro, 10), rank.astype(jnp.int32).reshape(micro, 8, 1, toks), cols


def solution(mesh):
    ep_size = mesh.shape['ep']
    sub_size = mesh.shape['sub']
    tok_spec = P(('dp', 'ep', 'sub'), None, None)
    route_spec = P(None, ('dp', 'ep', 'sub'), None)
    exp_spec = P(('ep', 'sub'), None, None)

    def device_body(input_a, input_b, route_idx, route_gate, attn_norm, w_query, w_key, w_value, w_out, moe_norm, w_gate, w_up, w_down):
        micro, toks, _ = route_idx.shape
        table = local_table(route_idx, route_gate, ep_size, sub_size * w_gate.shape[0])
        offs, rank_rows, cols = route_tables(table, micro, toks, ep_size, sub_size, w_gate.shape[0])
        peer_gate, peer_up, peer_down = to_core(w_gate), to_core(w_up), to_core(w_down)
        attend = functools.partial(attention_block, attn_norm=attn_norm, w_query=w_query, w_key=w_key, w_value=w_value, w_out=w_out, moe_norm=moe_norm)

        def gather_near(z):
            top, bot = z[:toks // 2], z[toks // 2:]
            y_top, x_bot = to_y(top), to_x(bot)
            return top, bot, to_x(top), x_bot, y_top, to_y(bot)

        def gather_far(near, *others):
            y_top, x_bot = lax.optimization_barrier((near[4], near[3]) + others)[:2]
            return near + (to_x(y_top), to_y(x_bot))

        weights = ((w_gate, w_up), (peer_gate, peer_up))

        def experts_in(m, nodes, starts, parts):
            return expert_in(nodes, starts, rank_rows[m], parts, sum((weights[n] for n in nodes), ()))

        def experts_out(m, chunk, starts, *u_parts):
            send_x, keep_x, send_y, keep_y = expert_out(chunk, starts, cols[m], u_parts, w_down, peer_down)
            return keep_x, keep_y, to_x(send_x), to_y(send_y), send_x

        def forward(sent):
            keep_x, keep_y, got_x, got_y, _ = sent
            return keep_x[1] + got_x[1], keep_y[1] + got_y[1]

        def arrive(forwards):
            rest_x, rest_y = forwards
            return to_y(rest_x), to_x(rest_y)

        def finish(hidden, sents, arrived):
            pieces = []
            for (keep_x, keep_y, got_x, got_y, _), (rest_x, rest_y) in zip(sents, arrived):
                pieces.append((keep_x[0] + got_x[0]) + rest_x)
                pieces.append((keep_y[0] + got_y[0]) + rest_y)
            width = pieces[0].shape[1]
            done = [(hidden[:, n * width:(n + 1) * width].astype(jnp.float32) + piece).astype(jnp.bfloat16) for n, piece in enumerate(pieces)]
            return jnp.concatenate(done, axis=1)[None]

        hidden_a, z_a = attend(after(input_a[0], table))
        near_a = gather_near(z_a)
        parts_a = []

        def far_of_a(q_heads, k_heads, v_heads):
            parts_a.append(gather_far(near_a, q_heads, k_heads, v_heads))
            return after(q_heads, near_a[4], near_a[3]), parts_a[0][6:]

        hidden_b, z_b = attend(after(input_b[0], z_a, offs, rank_rows, cols), ahead=far_of_a)
        near_b = gather_near(z_b)
        starts_a = after(offs[0], z_b)
        u_a = experts_in(0, (0, 1), starts_a, parts_a[0])
        parts_b = gather_far(near_b, u_a)
        starts_a0 = after(starts_a, u_a, near_b[4], near_b[3])
        sent_a0 = experts_out(0, 0, starts_a0, u_a)
        sent_a1 = experts_out(0, 1, after(starts_a0, sent_a0[-1], *parts_b[6:]), u_a)
        starts_b = after(offs[1], sent_a1[-1])
        u_b0 = experts_in(1, (0,), starts_b, parts_b)
        forward_a0 = forward(sent_a0)
        starts_b = after(starts_b, u_b0, *forward_a0)
        u_b1 = experts_in(1, (1,), starts_b, parts_b)
        forward_a1 = forward(sent_a1)
        arrived_a0 = arrive(forward_a0)
        starts_b = after(starts_b, u_b1, *forward_a1, *arrived_a0)
        sent_b0 = experts_out(1, 0, starts_b, u_b0, u_b1)
        arrived_a1 = arrive(forward_a1)
        starts_b = after(starts_b, sent_b0[-1], *arrived_a1)
        sent_b1 = experts_out(1, 1, starts_b, u_b0, u_b1)
        arrived_b = [arrive(forward(sent_b0)), arrive(forward(sent_b1))]
        return finish(hidden_a, [sent_a0, sent_a1], [arrived_a0, arrived_a1]), finish(hidden_b, [sent_b0, sent_b1], arrived_b)

    return jax.shard_map(device_body, mesh=mesh, in_specs=(tok_spec, tok_spec, route_spec, route_spec, P(), P(), P(), P(), P(), P(), exp_spec, exp_spec, exp_spec), out_specs=(tok_spec, tok_spec), check_vma=False)
```
